256 devices in a mesh: groups: 2 (over y), blk: 128 (over z, x, core).
Axes of the slice: x: 4, y: 2, z: 16, core: 2. Of those that a mesh axis runs over, the one named last changes fastest.
The devices are a block of a 4x16x16 slice.
Arguments:
- positions: float32 [3, 65536], P(None, ('groups', 'blk')), parts along dimension 1, may hold values from 0 to 96
- right_side: float32 [3, 65536], P(None, ('groups', 'blk')), parts along dimension 1, may hold values from -18 to 18
- neighbours: int32 [16, 65536], P(None, ('groups', 'blk')), parts along dimension 1, may hold values from 0 to 32767, as said below
- counts: int32 [65536], P(('groups', 'blk')), parts along dimension 0, may hold values from 1 to 16
Outputs:
- solution: float32 [3, 65536], P(None, ('groups', 'blk')), parts along dimension 1
- residual: float32 [3, 65536], P(None, ('groups', 'blk')), parts along dimension 1
The draws below stay inside these ranges and needn't reach their ends.
There are 2 independent parts, one for each index of `groups`. The reference program is written for one: setup_inputs(seed, part) draws one part's arguments, and reference() takes and returns one part's arrays. A program takes and returns all parts, laid end to end along the dimension named above; each array names one. Nothing has to cross between parts.
Inputs may be any that keep to these rules, and one draw needn't show every extreme that they name: `neighbours`: every entry in column i lies within 32 of i, counted cyclically over the 32768 particles.
All inputs are finite; a program needn't handle non-finite values.
Results may differ from the reference program's by a relative error of at most 0.0003.
Values sent between devices are 32-bit elements; how exact they have to be, the bound alone decides.
A program may use at most 64 MiB of HBM per device.

```python
import math
import jax
import jax.numpy as jnp
from jax import lax

NBR = 16
REACH = 32
ITERS = 2
NPART = 32768


wall = 96.0


def draw_positions(key, part):
    first, second = jax.random.split(jax.random.fold_in(key, 11))
    start = jax.random.uniform(first, (3, 1), jnp.float32, 10.0, 86.0)
    moves = jnp.clip(jax.random.normal(second, (3, NPART), jnp.float32) * 1.45, -6.0, 6.0)
    path = start + jnp.cumsum(moves, axis=1)
    folded = jnp.remainder(path, 2.0 * wall)
    return jnp.clip(wall - jnp.abs(wall - folded), 0.0, wall)


def draw_right_side(key, part):
    inner = jax.random.fold_in(key, 23)
    scale = 1.0 + 2.0 * jnp.arange(NPART, dtype=jnp.float32) / NPART
    values = jnp.clip(jax.random.normal(inner, (3, NPART), jnp.float32), -6.0, 6.0)
    return values * scale[None, :]


def draw_neighbours(key, part):
    inner = jax.random.fold_in(key, 37)
    offset = jax.random.randint(inner, (NBR, NPART), -REACH, REACH + 1, dtype=jnp.int32)
    own = jnp.arange(NPART, dtype=jnp.int32)
    return jnp.remainder(own[None, :] + offset, NPART).astype(jnp.int32)


def place_ends(array, rng, low, top_value):
    spot = [jax.random.randint(jax.random.fold_in(rng, axis), (), 0, length) for axis, length in enumerate(array.shape)]
    widest = array.shape.index(max(array.shape))
    neighbour = spot[:widest] + [(spot[widest] + 1) % array.shape[widest]] + spot[widest + 1:]
    return array.at[tuple(spot)].set(low).at[tuple(neighbour)].set(top_value)


def setup_inputs(seed: int = 0, part: int = 0) -> dict:
    key_of = jax.random.split(jax.random.key(seed), 5)
    part_splits = jax.random.split(jax.random.fold_in(key_of[4], part), 5)
    positions = draw_positions(jax.random.fold_in(jax.random.fold_in(key_of[4], part), 71), part)
    right_side = draw_right_side(jax.random.fold_in(jax.random.fold_in(key_of[4], part), 71), part)
    neighbours = draw_neighbours(jax.random.fold_in(jax.random.fold_in(key_of[4], part), 71), part)
    counts = place_ends(jax.random.randint(part_splits[3], (NPART,), 1, NBR + 1), jax.random.fold_in(part_splits[3], 1), 1, NBR).astype(jnp.int32)
    return dict(positions=positions, right_side=right_side, neighbours=neighbours, counts=counts)


SOFT = 0.0001
EPS = 1e-06

def pair_coefficients(dx, dy, dz):
    dist = jnp.sqrt(dx * dx + dy * dy + dz * dz + SOFT)
    inverse = 1.0 / dist
    cube = inverse * inverse * inverse
    correlation = dist < 2.0
    coef_a = jnp.where(correlation, 1.0 - 9.0 * dist / 32.0, 0.75 * inverse + 0.5 * cube)
    coef_b = jnp.where(correlation, 3.0 / 32.0 * inverse, 0.75 * cube - 1.5 * cube * inverse * inverse)
    return (coef_a, coef_b)

def far_tile(row_pos, col_pos, col_vec):
    dx = row_pos[0][:, None] - col_pos[0][None, :]
    dy = row_pos[1][:, None] - col_pos[1][None, :]
    dz = row_pos[2][:, None] - col_pos[2][None, :]
    coef_a, coef_b = pair_coefficients(dx, dy, dz)
    along = dx * col_vec[0][None, :] + dy * col_vec[1][None, :] + dz * col_vec[2][None, :]
    weighted = coef_b * along
    out_x = lax.optimization_barrier(jnp.sum(coef_a * col_vec[0][None, :] + weighted * dx, axis=1))
    out_y = lax.optimization_barrier(jnp.sum(coef_a * col_vec[1][None, :] + weighted * dy, axis=1))
    out_z = lax.optimization_barrier(jnp.sum(coef_a * col_vec[2][None, :] + weighted * dz, axis=1))
    return jnp.stack([out_x, out_y, out_z])

def far_field(positions, vec):
    total = positions.shape[1]
    size = total if total <= 512 else math.gcd(total, 512)
    count = total // size
    row_blocks = positions.reshape(3, count, size).transpose(1, 0, 2)
    result = lax.map(lambda rows: far_tile(rows, positions, vec), row_blocks)
    return result.transpose(1, 0, 2).reshape(3, total)

def lubrication(positions, vec, near_pos, near_vec, live):
    delta = positions[:, None, :] - near_pos
    square = lax.optimization_barrier(jnp.sum(delta * delta, axis=0)) + SOFT
    dist = jnp.sqrt(square)
    strength = live / ((0.5 + jnp.abs(dist - 2.0)) * square)
    along = lax.optimization_barrier(jnp.sum(delta * (vec[:, None, :] - near_vec), axis=0))
    return lax.optimization_barrier(jnp.sum(delta * (strength * along)[None], axis=1))

def reference(positions, right_side, neighbours, counts):
    slots = jnp.arange(neighbours.shape[0], dtype=jnp.int32)
    live = (slots[:, None] < counts[None, :]).astype(jnp.float32)
    near_pos = jnp.take(positions, neighbours, axis=1)

    def operator(vec):
        near_vec = jnp.take(vec, neighbours, axis=1)
        return far_field(positions, vec) + lubrication(positions, vec, near_pos, near_vec, live)
    beta = jnp.sqrt(jnp.sum(right_side * right_side) + EPS)
    basis = [right_side / beta]
    images = []
    cosines = []
    sines = []
    rotated = [beta]
    columns = []
    for step in range(ITERS):
        work = operator(basis[step])
        images.append(work)
        column = []
        for j in range(step + 1):
            entry = jnp.sum(work * basis[j])
            work = work - entry * basis[j]
            column.append(entry)
        below = jnp.sqrt(jnp.sum(work * work) + EPS)
        basis.append(work / below)
        column.append(below)
        for j in range(step):
            first, second = (column[j], column[j + 1])
            column[j] = cosines[j] * first + sines[j] * second
            column[j + 1] = -sines[j] * first + cosines[j] * second
        pivot = jnp.sqrt(column[step] * column[step] + below * below)
        cosines.append(column[step] / pivot)
        sines.append(below / pivot)
        column[step] = pivot
        rotated.append(-sines[step] * rotated[step])
        rotated[step] = cosines[step] * rotated[step]
        columns.append(column)
    coeffs = [None] * ITERS
    for step in reversed(range(ITERS)):
        accum = rotated[step]
        for j in range(step + 1, ITERS):
            accum = accum - columns[j][step] * coeffs[j]
        coeffs[step] = accum / columns[step][step]
    solution = jnp.zeros_like(right_side)
    residual = right_side
    for step in range(ITERS):
        solution = solution + coeffs[step] * basis[step]
        residual = residual - coeffs[step] * images[step]
    return (solution, residual)
```

```python
import functools
import math

import jax
import jax.numpy as jnp
from jax import lax
from jax.experimental import pallas as pl
from jax.experimental.pallas import tpu as pltpu
from jax.sharding import Mesh
from jax.sharding import PartitionSpec as P

REACH = 32
AXES = ("blk_0", "blk_1", "blk_2")
GROUPS_BLK = ("groups",) + AXES
MESH = pl.DeviceIdType.MESH
F32, BF16 = jnp.float32, jnp.bfloat16

SOFT = 0.0001
EPS = 1e-06
G = math.sqrt(0.75)
EDGE = 2.0 * G
FACT_A = 0.375 * G
FACT_B = 1.125 * G

RING = 12
CHUNK = 32


def hop(k):
    return ((k + 1) // 2) * (2 * (k % 2) - 1)


def total_of(x):
    return jnp.sum(jnp.sum(x, axis=1, keepdims=True), axis=0, keepdims=True)


def limbs(x, count):
    parts = []
    for k in range(count):
        part = x.astype(BF16)
        parts.append(part)
        if k < count - 1:
            x = x - part.astype(F32)
    return parts


def kernel(
    sizes, rows,
    pos_ref, rhs_ref, nbr_ref, cnt_ref,
    sol_ref, res_ref, a_hbm,
    blk, vec, red_c, red_x, red_z,
    keep_b, ring, stage_0, stage_1, wst_0, wst_1, acc, mult, centre, scale, lub, tot,
    recv_1, send_z1, send_x1, send_c1,
    recv_2, send_z2, send_x2, send_c2,
    recv_3, send_3, ring_out, ring_in,
):
    nz, nx, nc = sizes
    span = nx * nc
    tiles = nz * span
    pairs = tiles // 2
    ppg = span // 2
    zi, xi, ci = (lax.axis_index(a) for a in AXES)
    me = (zi * nx + xi) * nc + ci
    total = tiles * rows
    zoff = lambda k: (zi + hop(k) + nz) % nz
    xoff = lambda k: (xi + hop(k) + nx) % nx
    index = lambda z, x, c: (z * nx + x) * nc + c
    plus = nz // 2

    def source(t):
        group, inner = t // span, t % span
        return index(zoff(group), xoff(inner // nc), (ci + inner % nc) % nc)

    barrier = pltpu.get_barrier_semaphore()
    near = []
    for step in sorted({1 % nz, nz - 1} - {0}):
        near.append({"blk_0": (zi + step) % nz})
    for step in range(1, nx):
        near.append({"blk_1": (xi + step) % nx})
    for step in range(1, nc):
        near.append({"blk_2": (ci + step) % nc})
    for peer in near:
        pl.semaphore_signal(barrier, inc=1, device_id=peer, device_id_type=MESH)

    ones = jnp.ones((1, rows), F32)
    blk[me] = jnp.concatenate(
        [pos_ref[...], rhs_ref[...], ones, jnp.zeros((1, rows), F32)], axis=0
    )
    middle = jnp.sum(pos_ref[...], axis=1, keepdims=True) * (1.0 / rows)
    centre[...] = jnp.concatenate(
        [jnp.broadcast_to(middle, (3, rows)), jnp.zeros((5, rows), F32)], axis=0
    )
    line = lax.broadcasted_iota(jnp.int32, (8, rows), 0)
    scale[...] = jnp.where(line < 3, G, 1.0).astype(F32)
    own = me * rows + lax.broadcasted_iota(jnp.int32, nbr_ref.shape, 1)
    slot = lax.broadcasted_iota(jnp.int32, nbr_ref.shape, 0)
    offset = (nbr_ref[...] - own + (REACH + total)) % total
    offset = jnp.where(slot < cnt_ref[...], offset, -1)
    for o in range(2 * REACH + 1):
        mult[o : o + 1, :] = jnp.sum(
            jnp.where(offset == o, 1.0, 0.0), axis=0, keepdims=True
        )
    mult[2 * REACH + 1 :, :] = jnp.zeros((mult.shape[0] - 2 * REACH - 1, rows), F32)
    acc[...] = jnp.zeros(acc.shape, F32)

    pl.semaphore_wait(barrier, len(near))

    def copy(buf, s, send, recv, peer):
        return pltpu.make_async_remote_copy(
            src_ref=buf.at[s], dst_ref=buf.at[s], send_sem=send, recv_sem=recv.at[s],
            device_id=peer, device_id_type=MESH,
        )

    here = {"blk_0": zi}
    up = {"blk_0": (zi + 1) % nz}
    down = {"blk_0": (zi + nz - 1) % nz}

    def x_copies(buf, s, send, recv, g):
        return [
            copy(buf, s, send.at[g, k - 1], recv, {"blk_1": xoff(k)}) for k in range(1, nx)
        ]

    def c_copies(buf, s, send, recv, g, k):
        return [copy(buf, s, send.at[g, k], recv, {"blk_2": (ci + 1) % nc})]

    def arrived(buf, s, send, recv):
        copy(buf, s, send, recv, up).wait_recv()

    def at_z(g):
        return index(zoff(g), xi, ci)

    def spread_z(buf, send_x, send_c, recv, g):
        for c in x_copies(buf, at_z(g), send_x, recv, g):
            c.start()
        for c in c_copies(buf, at_z(g), send_c, recv, g, 0):
            c.start()

    def spread_x(buf, send_x, send_c, recv, g):
        for k in range(1, nx):
            s = index(zoff(g), xoff(k), ci)
            arrived(buf, s, send_x.at[g, 0], recv)
            for c in c_copies(buf, s, send_c, recv, g, k):
                c.start()

    def wait_c(buf, send_c, recv, g):
        for k in range(nx):
            s = index(zoff(g), xoff(k), (ci + 1) % nc)
            arrived(buf, s, send_c.at[g, 0], recv)

    def relay_z(g):
        s = at_z(g)
        arrived(blk, s, send_z1.at[0], recv_1)
        j = (g + 1) // 2

        @pl.when((g % 2 == 1) & (j < plus))
        def _():
            copy(blk, s, send_z1.at[g + 1], recv_1, down).start()

        @pl.when((g % 2 == 0) & (j < nz - 1 - plus))
        def _():
            copy(blk, s, send_z1.at[g + 1], recv_1, up).start()

        spread_z(blk, send_x1, send_c1, recv_1, g)

    def finish_sends(buf, send_x, send_c, recv):
        def body(g, _):
            s = at_z(g)
            for c in x_copies(buf, s, send_x, recv, g):
                c.wait_send()
            for k in range(nx):
                for c in c_copies(buf, s, send_c, recv, g, k):
                    c.wait_send()
            return 0

        lax.fori_loop(0, nz, body, 0)

    own_row = (blk[me] - centre[...]) * scale[...]
    xs = [own_row[c : c + 1, :] for c in range(3)]

    def centred(s):
        return (blk[s] - centre[...]) * scale[...]

    def weights(block, vectors, out):
        along = sum(block[c : c + 1, :] * vectors[c] for c in range(3))
        columns = [
            jnp.broadcast_to(v, (8, rows)) * block for v in vectors + [along]
        ]
        for k, part in enumerate(limbs(jnp.concatenate(columns, axis=0), 3)):
            out[32 * k : 32 * (k + 1), :] = part

    def coefficients(t, half, stage, out, slot, masked):
        s = source(t)
        block = centred(s)
        raw = blk[s]
        weights(block, [raw[3 + c : 4 + c, :] for c in range(3)], out)
        turned = block.T
        for j in range(rows // CHUNK):
            part = slice(j * CHUNK, (j + 1) * CHUNK)
            dx, dy, dz = (turned[part, c : c + 1] - xs[c] for c in range(3))
            square = (dx * dx + dy * dy) + (dz * dz + SOFT * 0.75)
            q = lax.rsqrt(square)
            q_far = jnp.minimum(q, 1.0 / EDGE)
            q2 = q_far * q_far
            a = q_far * (q2 + 2.0) + jnp.maximum(EDGE - square * q, 0.0)
            b = (q * q2) * (2.0 / 3.0 - q2)
            if masked:
                first = lax.broadcasted_iota(jnp.int32, b.shape, 0) + j * CHUNK
                second = lax.broadcasted_iota(jnp.int32, b.shape, 1)
                b = jnp.where(first == second, 0.0, b)
            for k, piece in enumerate(limbs(a, 2)):
                stage[k, part, :] = piece
                ring[slot, 2 * half + k, part, :] = piece
            for k, piece in enumerate(limbs(b, 3)):
                stage[2 + k, part, :] = piece
                keep_b[t, k, part, :] = piece

    def dot(w, m):
        return jnp.dot(w, m, preferred_element_type=F32)

    def product(w, a_parts, b_parts):
        acc[0] += dot(w, a_parts[0]) + dot(w, a_parts[1])
        acc[1] += dot(w, b_parts[0]) + dot(w, b_parts[1]) + dot(w, b_parts[2])

    def staged(stage, out):
        product(out[...], [stage[k] for k in range(2)], [stage[2 + k] for k in range(3)])

    def ring_write(p):
        return pltpu.make_async_copy(ring.at[p % RING], a_hbm.at[p], ring_out.at[p % RING])

    def ring_read(p):
        return pltpu.make_async_copy(a_hbm.at[p], ring.at[p % RING], ring_in.at[p % RING])

    copy(blk, me, send_z1.at[0], recv_1, up).start()
    copy(blk, me, send_z1.at[1], recv_1, down).start()
    spread_z(blk, send_x1, send_c1, recv_1, 0)

    def pair(p, masked):
        slot = p % RING
        coefficients(2 * p, 0, stage_0, wst_0, slot, masked)
        staged(stage_0, wst_0)
        coefficients(2 * p + 1, 1, stage_1, wst_1, slot, False)

    coefficients(0, 0, stage_0, wst_0, 0, True)
    staged(stage_0, wst_0)
    spread_x(blk, send_x1, send_c1, recv_1, 0)
    wait_c(blk, send_c1, recv_1, 0)
    relay_z(1)
    coefficients(1, 1, stage_1, wst_1, 0, False)

    def first(p, _):
        g = p // ppg

        @pl.when((p % ppg == 0) & (g + 1 < nz))
        def _():
            relay_z(g + 1)

        @pl.when(p % ppg == 0)
        def _():
            spread_x(blk, send_x1, send_c1, recv_1, g)
            wait_c(blk, send_c1, recv_1, g)

        @pl.when(p >= RING)
        def _():
            ring_write(p - RING).wait()

        staged(stage_1, wst_1)
        coefficients(2 * p, 0, stage_0, wst_0, p % RING, False)
        staged(stage_0, wst_0)
        coefficients(2 * p + 1, 1, stage_1, wst_1, p % RING, False)
        ring_write(p - 1).start()
        return 0

    lax.fori_loop(1, pairs, first, 0)
    staged(stage_1, wst_1)

    def sums():
        out = []
        for k in range(2):
            parts = acc[k]
            out.append((parts[0:32] + parts[32:64]) + parts[64:96])
        a, b = out
        row = lambda m, r: m[r : r + 1, :]
        bv = [row(b, 8 * c + 6) for c in range(3)]
        along = sum(xs[c] * bv[c] for c in range(3)) - row(b, 30)
        far = []
        for k in range(3):
            cross = sum(xs[c] * row(b, 8 * c + k) for c in range(3))
            far.append(
                FACT_A * row(a, 8 * k + 6)
                + FACT_B * ((xs[k] * along - cross) + row(b, 24 + k))
            )
        return far

    before, after = (me + tiles - 1) % tiles, (me + 1) % tiles

    def lubricated(rows_of):
        def six(s):
            return jnp.concatenate([blk[s][0:3, :]] + rows_of(s), axis=0)

        wide = jnp.concatenate([six(before), six(me), six(after)], axis=1)
        mine = six(me)
        for o in range(2 * REACH + 1):
            begin = rows + o - REACH
            delta = mine - wide[:, begin : begin + rows]
            for k in range(6):
                lub[k, o : o + 1, :] = delta[k : k + 1, :]
        for k in range(6):
            lub[k, 2 * REACH + 1 :, :] = jnp.zeros((lub.shape[1] - 2 * REACH - 1, rows), F32)
        d = [lub[k] for k in range(3)]
        e = [lub[3 + k] for k in range(3)]
        square = d[0] * d[0] + d[1] * d[1] + d[2] * d[2] + SOFT
        dist = jnp.sqrt(square)
        strength = mult[...] / ((0.5 + jnp.abs(dist - 2.0)) * square)
        force = strength * (d[0] * e[0] + d[1] * e[1] + d[2] * e[2])
        return [jnp.sum(force * d[k], axis=0, keepdims=True) for k in range(3)]

    rhs = [rhs_ref[k : k + 1, :] for k in range(3)]
    far = sums()
    near_part = lubricated(lambda s: [blk[s][3:6, :]])
    work = [far[k] + near_part[k] for k in range(3)]
    inner = lambda u, v: total_of(u[0] * v[0] + u[1] * v[1] + u[2] * v[2])
    lane = lax.broadcasted_iota(jnp.int32, (1, rows), 1)

    def packed(values):
        line = jnp.zeros((1, rows), F32)
        for k, value in enumerate(values):
            line = jnp.where(lane == k, value, line)
        return line

    def unpacked(line, count):
        return [
            jnp.sum(jnp.where(lane[:, : line.shape[1]] == k, line, 0.0), axis=1, keepdims=True)
            for k in range(count)
        ]

    vec[me] = jnp.concatenate(
        work + [packed([inner(rhs, rhs), inner(work, rhs), inner(work, work)])], axis=0
    )

    def last_writes(p, _):
        ring_write(p).wait()
        return 0

    ring_write(pairs - 1).start()
    lax.fori_loop(max(pairs - RING, 0), pairs, last_writes, 0)
    for p in range(min(RING, pairs)):
        ring_read(p).start()

    def z_copy(k):
        return copy(vec, me, send_z2.at[k], recv_2, {"blk_0": zoff(k)})

    def z_start(k, _):
        z_copy(k).start()
        return 0

    lax.fori_loop(1, nz, z_start, 0)
    spread_z(vec, send_x2, send_c2, recv_2, 0)
    acc[...] = jnp.zeros(acc.shape, F32)
    tot[...] = jnp.zeros(tot.shape, F32)

    LOOK_Z, LOOK_X = 4, 2

    def far_stage(g):
        arrived(vec, at_z(g), send_z2.at[0], recv_2)
        spread_z(vec, send_x2, send_c2, recv_2, g)

    def mid_stage(g):
        spread_x(vec, send_x2, send_c2, recv_2, g)

    def group(g, _):
        @pl.when(g + LOOK_Z < nz)
        def _():
            far_stage(g + LOOK_Z)

        @pl.when(g + LOOK_X < nz)
        def _():
            mid_stage(g + LOOK_X)

        wait_c(vec, send_c2, recv_2, g)

        def second(i, _):
            p = g * ppg + i
            ring_read(p).wait()
            for half in range(2):
                t = 2 * p + half
                s = source(t)
                v = vec[s]
                tot[...] += v
                out = wst_0 if half == 0 else wst_1
                weights(centred(s), [v[c : c + 1, :] for c in range(3)], out)
                product(
                    out[...],
                    [ring[p % RING, 2 * half + k] for k in range(2)],
                    [keep_b[t, k] for k in range(3)],
                )

            @pl.when(p + RING < pairs)
            def _():
                ring_read(p + RING).start()

            return 0

        lax.fori_loop(0, ppg, second, 0)
        return 0

    mid_stage(0)
    for g in range(1, min(LOOK_Z, nz)):
        far_stage(g)
    for g in range(1, min(LOOK_X, nz)):
        mid_stage(g)
    lax.fori_loop(0, nz, group, 0)

    far = sums()
    near_part = lubricated(lambda s: [vec[s][0:3, :]])
    again = [far[k] + near_part[k] for k in range(3)]

    rr, wr, ww = unpacked(tot[3:4, :], 3)
    beta = jnp.sqrt(rr + EPS)
    image_0 = [work[k] / beta for k in range(3)]
    v_0 = [rhs[k] / beta for k in range(3)]
    h_00 = wr / (beta * beta)
    h_10 = jnp.sqrt(ww / (beta * beta) - h_00 * h_00 + EPS)
    v_1 = [(image_0[k] - h_00 * v_0[k]) / h_10 for k in range(3)]
    image_1 = [(again[k] / beta - h_00 * image_0[k]) / h_10 for k in range(3)]
    line = packed([inner(image_1, v_0), inner(image_1, v_1), inner(image_1, image_1)])[:, :128]

    def summed(buf, mine, count, peers, first_sem):
        buf[mine] = line
        copies = [
            pltpu.make_async_remote_copy(
                src_ref=buf.at[mine], dst_ref=buf.at[mine],
                send_sem=send_3.at[first_sem + k], recv_sem=recv_3.at[first_sem + mine],
                device_id=peer, device_id_type=MESH,
            )
            for k, peer in enumerate(peers)
        ]
        for c in copies:
            c.start()
        return copies

    def collected(buf, mine, count, copies, others, first_sem):
        for k, other in enumerate(others):
            pltpu.make_async_remote_copy(
                src_ref=buf.at[mine], dst_ref=buf.at[other],
                send_sem=send_3.at[first_sem + k], recv_sem=recv_3.at[first_sem + other],
                device_id=up, device_id_type=MESH,
            ).wait_recv()
        out = buf[0]
        for k in range(1, count):
            out = out + buf[k]
        for c in copies:
            c.wait_send()
        return out

    base = 0
    for buf, mine, count, name in (
        (red_c, ci, nc, "blk_2"), (red_x, xi, nx, "blk_1"), (red_z, zi, nz, "blk_0")
    ):
        others = [(mine + k) % count for k in range(1, count)]
        copies = summed(buf, mine, count, [{name: o} for o in others], base)
        line = collected(buf, mine, count, copies, others, base)
        base += count
    h_01, h_11, squares = unpacked(line, 3)
    h_21 = jnp.sqrt(squares - h_01 * h_01 - h_11 * h_11 + EPS)

    rho_0 = jnp.sqrt(h_00 * h_00 + h_10 * h_10)
    c_0, s_0 = h_00 / rho_0, h_10 / rho_0
    g_1 = -s_0 * beta
    g_0 = c_0 * beta
    r_01 = c_0 * h_01 + s_0 * h_11
    r_11 = c_0 * h_11 - s_0 * h_01
    rho_1 = jnp.sqrt(r_11 * r_11 + h_21 * h_21)
    g_1 = (r_11 / rho_1) * g_1
    y_1 = g_1 / rho_1
    y_0 = (g_0 - r_01 * y_1) / rho_0
    for k in range(3):
        sol_ref[k : k + 1, :] = y_0 * v_0[k] + y_1 * v_1[k]
        res_ref[k : k + 1, :] = rhs[k] - y_0 * image_0[k] - y_1 * image_1[k]

    def z_done(k, _):
        z_copy(k).wait_send()
        return 0

    lax.fori_loop(1, nz, z_done, 0)
    copy(blk, me, send_z1.at[0], recv_1, up).wait_send()
    copy(blk, me, send_z1.at[1], recv_1, down).wait_send()

    def relay_done(g, _):
        j = (g + 1) // 2

        @pl.when(((g % 2 == 1) & (j < plus)) | ((g % 2 == 0) & (j < nz - 1 - plus)))
        def _():
            copy(blk, me, send_z1.at[g + 1], recv_1, up).wait_send()

        return 0

    lax.fori_loop(1, nz, relay_done, 0)
    finish_sends(blk, send_x1, send_c1, recv_1)
    finish_sends(vec, send_x2, send_c2, recv_2)


def on_device(positions, right_side, neighbours, counts):
    rows = positions.shape[1]
    sizes = nz, nx, nc = tuple(lax.axis_size(a) for a in AXES)
    tiles = nz * nx * nc
    slots = 8 * -(-(2 * REACH + 1) // 8)
    vmem = pl.BlockSpec(memory_space=pltpu.VMEM)
    dma = pltpu.SemaphoreType.DMA
    small = jax.ShapeDtypeStruct((3, rows), F32)
    gather_sems = [dma((tiles,)), dma((nz + 2,)), dma((nz, max(nx - 1, 1))), dma((nz, nx))]
    out = pl.pallas_call(
        functools.partial(kernel, sizes, rows),
        out_shape=(small, small, jax.ShapeDtypeStruct((tiles // 2, 4, rows, rows), BF16)),
        in_specs=[vmem] * 4,
        out_specs=(vmem, vmem, pl.BlockSpec(memory_space=pltpu.HBM)),
        scratch_shapes=[
            pltpu.VMEM((tiles, 8, rows), F32),
            pltpu.VMEM((tiles, 4, rows), F32),
            pltpu.VMEM((nc, 1, 128), F32),
            pltpu.VMEM((nx, 1, 128), F32),
            pltpu.VMEM((nz, 1, 128), F32),
            pltpu.VMEM((tiles, 3, rows, rows), BF16),
            pltpu.VMEM((RING, 4, rows, rows), BF16),
            pltpu.VMEM((5, rows, rows), BF16),
            pltpu.VMEM((5, rows, rows), BF16),
            pltpu.VMEM((96, rows), BF16),
            pltpu.VMEM((96, rows), BF16),
            pltpu.VMEM((2, 96, rows), F32),
            pltpu.VMEM((slots, rows), F32),
            pltpu.VMEM((8, rows), F32),
            pltpu.VMEM((8, rows), F32),
            pltpu.VMEM((6, slots, rows), F32),
            pltpu.VMEM((4, rows), F32),
        ]
        + gather_sems * 2
        + [dma((nz + nx + nc,)), dma((nz + nx + nc,)), dma((RING,)), dma((RING,))],
        compiler_params=pltpu.CompilerParams(
            collective_id=0, has_side_effects=True, vmem_limit_bytes=67043328
        ),
    )(positions, right_side, neighbours, counts[None, :])
    return out[0], out[1]


def solution(mesh):
    torus = Mesh(mesh.devices.reshape(mesh.shape["groups"], 16, 4, 2), GROUPS_BLK)
    placed = (P(None, GROUPS_BLK), P(None, GROUPS_BLK), P(None, GROUPS_BLK), P(GROUPS_BLK))
    return jax.shard_map(
        on_device,
        mesh=torus,
        in_specs=placed,
        out_specs=(P(None, GROUPS_BLK), P(None, GROUPS_BLK)),
        check_vma=False,
    )
```

```python
import functools
import math

import jax
import jax.numpy as jnp
from jax import lax
from jax.experimental import pallas as pl
from jax.experimental.pallas import tpu as pltpu
from jax.sharding import Mesh
from jax.sharding import PartitionSpec as P

REACH = 32
AXES = ("blk_0", "blk_1", "blk_2")
GROUPS_BLK = ("groups",) + AXES
MESH = pl.DeviceIdType.MESH
F32, BF16 = jnp.float32, jnp.bfloat16

SOFT = 0.0001
EPS = 1e-06
G = math.sqrt(0.75)
EDGE = 2.0 * G
FACT_A = 0.375 * G
FACT_B = 1.125 * G

RING = 4
CHUNK = 32
LOOK_Z, LOOK_X = 6, 2


def hop(k):
    return lax.div(k + 1, 2) * (2 * lax.rem(k, 2) - 1)


def total_of(x):
    return jnp.sum(jnp.sum(x, axis=1, keepdims=True), axis=0, keepdims=True)


def limbs(x, count):
    parts = []
    for k in range(count):
        part = x.astype(BF16)
        parts.append(part)
        if k < count - 1:
            x = x - part.astype(F32)
    return parts


def kernel(
    sizes, rows,
    pos_ref, rhs_ref, nbr_ref, cnt_ref,
    out_ref, a_hbm,
    blk, vec, red_c, red_x, red_z,
    keep_b, ring, stage_0, stage_1, wst_0, wst_1, acc, mult, centre, scale, lub, tot,
    recv_1, core_1, send_z1, send_x1, send_c1,
    recv_2, core_2, send_z2, send_x2, send_c2,
    recv_3, send_3, ring_out, ring_in,
):
    nz, nx, nc = sizes
    span = nx * nc
    tiles = nz * span
    zi, xi, ci = (lax.axis_index(a) for a in AXES)
    total = tiles * rows
    order = (zi * nx + xi) * nc + ci
    zat = lambda k: lax.rem(zi + hop(k) + nz, nz)
    xat = [lax.rem(xi + k, nx) for k in range(nx)]
    cat = [lax.rem(ci + k, nc) for k in range(nc)]
    at = lambda z, x, c: (z * nc + c) * nx + x
    me = at(zi, xi, ci)
    within = [cat[d] * nx + xat[k] for d in range(nc) for k in range(nx)]
    plus = nz // 2
    stages, wsts = (stage_0, stage_1), (wst_0, wst_1)

    barrier = pltpu.get_barrier_semaphore()
    near = []
    for step in sorted({1 % nz, nz - 1} - {0}):
        near.append({"blk_0": lax.rem(zi + step, nz)})
    near += [{"blk_1": x} for x in xat[1:]] + [{"blk_2": c} for c in cat[1:]]
    for peer in near:
        pl.semaphore_signal(barrier, inc=1, device_id=peer, device_id_type=MESH)

    ones = jnp.ones((1, rows), F32)
    blk[me] = jnp.concatenate(
        [pos_ref[...], rhs_ref[...], ones, jnp.zeros((1, rows), F32)], axis=0
    )
    middle = jnp.sum(pos_ref[...], axis=1, keepdims=True) * (1.0 / rows)
    centre[...] = jnp.concatenate(
        [jnp.broadcast_to(middle, (3, rows)), jnp.zeros((5, rows), F32)], axis=0
    )
    line = lax.broadcasted_iota(jnp.int32, (8, rows), 0)
    scale[...] = jnp.where(line < 3, G, 1.0).astype(F32)
    acc[...] = jnp.zeros(acc.shape, F32)
    pl.semaphore_wait(barrier, len(near))

    def copy(buf, s, send, recv, peer):
        return pltpu.make_async_remote_copy(
            src_ref=buf.at[s], dst_ref=buf.at[s], send_sem=send, recv_sem=recv,
            device_id=peer, device_id_type=MESH,
        )

    up = {"blk_0": lax.rem(zi + 1, nz)}
    down = {"blk_0": lax.rem(zi + nz - 1, nz)}
    beside = {"blk_2": cat[nc - 1]}

    def x_copies(buf, s, send, recv, g):
        return [
            copy(buf, s, send.at[g, k - 1], recv.at[s], {"blk_1": xat[k]}) for k in range(1, nx)
        ]

    def c_copy(buf, send, core, g, z, c):
        return copy(buf, pl.ds((z * nc + c) * nx, nx), send.at[g], core.at[z], beside)

    def z_stage(buf, send_x, recv, g, z):
        s = at(z, xi, ci)
        copy(buf, s, send_x.at[g, 0], recv.at[s], up).wait_recv()
        for c in x_copies(buf, s, send_x, recv, g):
            c.start()

    def x_stage(buf, send_x, send_c, recv, core, g, z):
        for k in range(1, nx):
            s = at(z, xat[k], ci)
            copy(buf, s, send_x.at[g, 0], recv.at[s], up).wait_recv()
        c_copy(buf, send_c, core, g, z, ci).start()

    def c_stage(buf, send_c, core, g, z):
        c_copy(buf, send_c, core, g, z, cat[nc - 1]).wait_recv()

    def relay(g, z):
        s = at(z, xi, ci)
        copy(blk, s, send_z1.at[0], recv_1.at[s], up).wait_recv()
        j, odd = lax.div(g + 1, 2), lax.rem(g, 2)

        @pl.when((odd == 1) & (j < plus))
        def _():
            copy(blk, s, send_z1.at[g + 1], recv_1.at[s], down).start()

        @pl.when((odd == 0) & (j < nz - 1 - plus))
        def _():
            copy(blk, s, send_z1.at[g + 1], recv_1.at[s], up).start()

        for c in x_copies(blk, s, send_x1, recv_1, g):
            c.start()

    def finish_sends(buf, send_x, send_c, recv, core):
        def body(g, _):
            for c in x_copies(buf, me, send_x, recv, g):
                c.wait_send()
            c_copy(buf, send_c, core, g, g, ci).wait_send()
            return 0

        lax.fori_loop(0, nz, body, 0)

    own_row = (blk[me] - centre[...]) * scale[...]
    xs = [own_row[c : c + 1, :] for c in range(3)]

    def centred(s):
        return (blk[s] - centre[...]) * scale[...]

    def weights(block, vectors, out):
        along = sum(block[c : c + 1, :] * vectors[c] for c in range(3))
        columns = [
            jnp.broadcast_to(v, (8, rows)) * block for v in vectors + [along]
        ]
        for k, part in enumerate(limbs(jnp.concatenate(columns, axis=0), 3)):
            out[32 * k : 32 * (k + 1), :] = part

    def coefficients(g, slot, n, s, masked):
        stage, t = stages[n % 2], g * span + n
        block = centred(s)
        raw = blk[s]
        weights(block, [raw[3 + c : 4 + c, :] for c in range(3)], wsts[n % 2])
        turned = block.T
        for j in range(rows // CHUNK):
            part = slice(j * CHUNK, (j + 1) * CHUNK)
            dx, dy, dz = (turned[part, c : c + 1] - xs[c] for c in range(3))
            square = (dx * dx + dy * dy) + (dz * dz + SOFT * 0.75)
            q = lax.rsqrt(square)
            q_far = jnp.minimum(q, 1.0 / EDGE)
            q2 = q_far * q_far
            a = q_far * (q2 + 2.0) + jnp.maximum(EDGE - square * q, 0.0)
            b = (q * q2) * (2.0 / 3.0 - q2)
            if masked:
                first = lax.broadcasted_iota(jnp.int32, b.shape, 0) + j * CHUNK
                second = lax.broadcasted_iota(jnp.int32, b.shape, 1)
                b = jnp.where(first == second, 0.0, b)
            for k, piece in enumerate(limbs(a, 2)):
                stage[k, part, :] = piece
                ring[slot, 2 * n + k, part, :] = piece
            for k, piece in enumerate(limbs(b, 3)):
                stage[2 + k, part, :] = piece
                keep_b[t, k, part, :] = piece

    def dot(w, m):
        return jnp.dot(w, m, preferred_element_type=F32)

    def staged(n):
        stage, w = stages[n % 2], wsts[n % 2][...]
        acc[0] += dot(w, stage[0]) + dot(w, stage[1])
        acc[1] += dot(w, stage[2]) + dot(w, stage[3]) + dot(w, stage[4])

    def ring_write(g):
        slot = lax.rem(g, RING)
        return pltpu.make_async_copy(ring.at[slot], a_hbm.at[g], ring_out.at[slot])

    def ring_read(g):
        slot = lax.rem(g, RING)
        return pltpu.make_async_copy(a_hbm.at[g], ring.at[slot], ring_in.at[slot])

    copy(blk, me, send_z1.at[0], recv_1.at[me], up).start()
    copy(blk, me, send_z1.at[1], recv_1.at[me], down).start()
    for c in x_copies(blk, me, send_x1, recv_1, 0):
        c.start()
    coefficients(0, 0, 0, me, True)

    own = order * rows + lax.broadcasted_iota(jnp.int32, nbr_ref.shape, 1)
    rank = lax.broadcasted_iota(jnp.int32, nbr_ref.shape, 0)
    offset = nbr_ref[...] - own + REACH
    offset = jnp.where(offset < 0, offset + total, offset)
    offset = jnp.where(offset >= total, offset - total, offset)
    offset = jnp.where(rank < cnt_ref[...], offset, -1)
    for o in range(2 * REACH + 1):
        mult[o : o + 1, :] = jnp.sum(
            jnp.where(offset == o, 1.0, 0.0), axis=0, keepdims=True
        )
    mult[2 * REACH + 1 :, :] = jnp.zeros((mult.shape[0] - 2 * REACH - 1, rows), F32)

    z_1, z_2, z_3 = (zat(jnp.int32(k)) for k in (1, 2, 3))
    relay(jnp.int32(1), z_1)
    relay(jnp.int32(2), z_2)
    x_stage(blk, send_x1, send_c1, recv_1, core_1, 0, zi)
    for n in range(1, nx):
        staged(n - 1)
        coefficients(0, 0, n, zi * span + within[n], False)
    x_stage(blk, send_x1, send_c1, recv_1, core_1, 1, z_1)
    c_stage(blk, send_c1, core_1, 0, zi)
    for n in range(nx, span):
        staged(n - 1)
        coefficients(0, 0, n, zi * span + within[n], False)

    def first(g, zs):
        z_0, z_1 = zs
        z_2 = zat(g + 2)

        @pl.when(g + 2 < nz)
        def _():
            relay(g + 2, z_2)

        @pl.when(g + 1 < nz)
        def _():
            x_stage(blk, send_x1, send_c1, recv_1, core_1, g + 1, z_1)

        c_stage(blk, send_c1, core_1, g, z_0)

        @pl.when(g >= RING)
        def _():
            ring_write(g - RING).wait()

        slot = lax.rem(g, RING)
        for n in range(span):
            staged(n - 1)
            coefficients(g, slot, n, z_0 * span + within[n], False)
            if n == 0:
                ring_write(g - 1).start()
        return z_1, z_2

    lax.fori_loop(1, nz, first, (z_1, z_2))
    staged(span - 1)

    def sums():
        out = []
        for k in range(2):
            parts = acc[k]
            out.append((parts[0:32] + parts[32:64]) + parts[64:96])
        a, b = out
        row = lambda m, r: m[r : r + 1, :]
        bv = [row(b, 8 * c + 6) for c in range(3)]
        along = sum(xs[c] * bv[c] for c in range(3)) - row(b, 30)
        far = []
        for k in range(3):
            cross = sum(xs[c] * row(b, 8 * c + k) for c in range(3))
            far.append(
                FACT_A * row(a, 8 * k + 6)
                + FACT_B * ((xs[k] * along - cross) + row(b, 24 + k))
            )
        return far

    def place(b):
        return at(lax.div(b, span), lax.rem(lax.div(b, nc), nx), lax.rem(b, nc))

    before = place(lax.rem(order + tiles - 1, tiles))
    after = place(lax.rem(order + 1, tiles))

    def lubricated(rows_of):
        def six(s):
            return jnp.concatenate([blk[s][0:3, :], rows_of(s)], axis=0)

        wide = jnp.concatenate([six(before), six(me), six(after)], axis=1)
        mine = six(me)
        for o in range(2 * REACH + 1):
            begin = rows + o - REACH
            delta = mine - wide[:, begin : begin + rows]
            for k in range(6):
                lub[k, o : o + 1, :] = delta[k : k + 1, :]
        for k in range(6):
            lub[k, 2 * REACH + 1 :, :] = jnp.zeros((lub.shape[1] - 2 * REACH - 1, rows), F32)
        d = [lub[k] for k in range(3)]
        e = [lub[3 + k] for k in range(3)]
        square = d[0] * d[0] + d[1] * d[1] + d[2] * d[2] + SOFT
        dist = jnp.sqrt(square)
        strength = mult[...] / ((0.5 + jnp.abs(dist - 2.0)) * square)
        force = strength * (d[0] * e[0] + d[1] * e[1] + d[2] * e[2])
        return [jnp.sum(force * d[k], axis=0, keepdims=True) for k in range(3)]

    rhs = [rhs_ref[k : k + 1, :] for k in range(3)]
    far = sums()
    near_part = lubricated(lambda s: blk[s][3:6, :])
    work = [far[k] + near_part[k] for k in range(3)]
    inner = lambda u, v: total_of(u[0] * v[0] + u[1] * v[1] + u[2] * v[2])
    lane = lax.broadcasted_iota(jnp.int32, (1, rows), 1)

    def packed(values):
        line = jnp.zeros((1, rows), F32)
        for k, value in enumerate(values):
            line = jnp.where(lane == k, value, line)
        return line

    def unpacked(line, count):
        return [
            jnp.sum(jnp.where(lane[:, : line.shape[1]] == k, line, 0.0), axis=1, keepdims=True)
            for k in range(count)
        ]

    vec[me] = jnp.concatenate(
        work + [packed([inner(rhs, rhs), inner(work, rhs), inner(work, work)])], axis=0
    )

    def z_copy(k):
        return copy(vec, me, send_z2.at[k], recv_2.at[me], {"blk_0": zat(k)})

    def z_start(k, _):
        z_copy(k).start()
        return 0

    for c in x_copies(vec, me, send_x2, recv_2, 0):
        c.start()
    lax.fori_loop(1, nz, z_start, 0)

    def last_writes(g, _):
        ring_write(g).wait()
        return 0

    ring_write(jnp.int32(nz - 1)).start()
    lax.fori_loop(max(nz - RING, 0), nz, last_writes, 0)
    for g in range(min(RING, nz)):
        ring_read(jnp.int32(g)).start()
    acc[...] = jnp.zeros(acc.shape, F32)
    tot[...] = jnp.zeros(tot.shape, F32)

    def z_second(g):
        z_stage(vec, send_x2, recv_2, g, zat(g))

    def x_second(g):
        x_stage(vec, send_x2, send_c2, recv_2, core_2, g, zat(g))

    def second(g, _):
        @pl.when(g + LOOK_Z < nz)
        def _():
            z_second(g + LOOK_Z)

        @pl.when(g + LOOK_X < nz)
        def _():
            x_second(g + LOOK_X)

        z_0 = zat(g)
        c_stage(vec, send_c2, core_2, g, z_0)
        ring_read(g).wait()
        slot = lax.rem(g, RING)
        sum_a = sum_b = None
        sum_v = tot[...]
        for n in range(span):
            s = z_0 * span + within[n]
            v = vec[s]
            sum_v = sum_v + v
            weights(centred(s), [v[c : c + 1, :] for c in range(3)], wsts[n % 2])
            w = wsts[n % 2][...]
            for k in range(2):
                part = dot(w, ring[slot, 2 * n + k])
                sum_a = part if sum_a is None else sum_a + part
            for k in range(3):
                part = dot(w, keep_b[g * span + n, k])
                sum_b = part if sum_b is None else sum_b + part
        tot[...] = sum_v
        acc[0] += sum_a
        acc[1] += sum_b

        @pl.when(g + RING < nz)
        def _():
            ring_read(g + RING).start()

        return 0

    z_second(jnp.int32(1))
    z_second(jnp.int32(2))
    x_second(jnp.int32(0))
    for g in range(3, min(LOOK_Z, nz)):
        z_second(jnp.int32(g))
    for g in range(1, min(LOOK_X, nz)):
        x_second(jnp.int32(g))
    lax.fori_loop(0, nz, second, 0)

    far = sums()
    near_part = lubricated(lambda s: vec[s][0:3, :])
    again = [far[k] + near_part[k] for k in range(3)]

    rr, wr, ww = unpacked(tot[3:4, :], 3)
    beta = jnp.sqrt(rr + EPS)
    image_0 = [work[k] / beta for k in range(3)]
    v_0 = [rhs[k] / beta for k in range(3)]
    h_00 = wr / (beta * beta)
    h_10 = jnp.sqrt(ww / (beta * beta) - h_00 * h_00 + EPS)
    v_1 = [(image_0[k] - h_00 * v_0[k]) / h_10 for k in range(3)]
    image_1 = [(again[k] / beta - h_00 * image_0[k]) / h_10 for k in range(3)]
    line = packed([inner(image_1, v_0), inner(image_1, v_1), inner(image_1, image_1)])[:, :128]

    base = 0
    for buf, mine, count, name in (
        (red_c, ci, nc, "blk_2"), (red_x, xi, nx, "blk_1"), (red_z, zi, nz, "blk_0")
    ):
        others = [lax.rem(mine + k, count) for k in range(1, count)]
        buf[mine] = line
        copies = [
            copy(buf, mine, send_3.at[base + k], recv_3.at[base + mine], {name: other})
            for k, other in enumerate(others)
        ]
        for c in copies:
            c.start()
        for k, other in enumerate(others):
            copy(buf, other, send_3.at[base + k], recv_3.at[base + other], up).wait_recv()
        line = buf[0]
        for k in range(1, count):
            line = line + buf[k]
        for c in copies:
            c.wait_send()
        base += count
    h_01, h_11, squares = unpacked(line, 3)
    h_21 = jnp.sqrt(squares - h_01 * h_01 - h_11 * h_11 + EPS)

    rho_0 = jnp.sqrt(h_00 * h_00 + h_10 * h_10)
    c_0, s_0 = h_00 / rho_0, h_10 / rho_0
    g_1 = -s_0 * beta
    g_0 = c_0 * beta
    r_01 = c_0 * h_01 + s_0 * h_11
    r_11 = c_0 * h_11 - s_0 * h_01
    rho_1 = jnp.sqrt(r_11 * r_11 + h_21 * h_21)
    g_1 = (r_11 / rho_1) * g_1
    y_1 = g_1 / rho_1
    y_0 = (g_0 - r_01 * y_1) / rho_0
    for k in range(3):
        out_ref[0, k : k + 1, :] = y_0 * v_0[k] + y_1 * v_1[k]
        out_ref[1, k : k + 1, :] = rhs[k] - y_0 * image_0[k] - y_1 * image_1[k]

    def z_done(k, _):
        z_copy(k).wait_send()
        return 0

    lax.fori_loop(1, nz, z_done, 0)

    def relay_done(g, _):
        copy(blk, me, send_z1.at[g], recv_1.at[me], up).wait_send()
        return 0

    lax.fori_loop(0, nz - 1, relay_done, 0)
    finish_sends(blk, send_x1, send_c1, recv_1, core_1)
    finish_sends(vec, send_x2, send_c2, recv_2, core_2)


def on_device(positions, right_side, neighbours, counts):
    rows = positions.shape[1]
    sizes = nz, nx, nc = tuple(lax.axis_size(a) for a in AXES)
    span = nx * nc
    tiles = nz * span
    slots = 8 * -(-(2 * REACH + 1) // 8)
    vmem = pl.BlockSpec(memory_space=pltpu.VMEM)
    dma = pltpu.SemaphoreType.DMA
    gather_sems = [dma((tiles,)), dma((nz,)), dma((nz + 1,)), dma((nz, nx - 1)), dma((nz,))]
    out, _ = pl.pallas_call(
        functools.partial(kernel, sizes, rows),
        out_shape=(
            jax.ShapeDtypeStruct((2, 3, rows), F32),
            jax.ShapeDtypeStruct((nz, 2 * span, rows, rows), BF16),
        ),
        in_specs=[vmem] * 4,
        out_specs=(vmem, pl.BlockSpec(memory_space=pltpu.HBM)),
        scratch_shapes=[
            pltpu.VMEM((tiles, 8, rows), F32),
            pltpu.VMEM((tiles, 4, rows), F32),
            pltpu.VMEM((nc, 1, 128), F32),
            pltpu.VMEM((nx, 1, 128), F32),
            pltpu.VMEM((nz, 1, 128), F32),
            pltpu.VMEM((tiles, 3, rows, rows), BF16),
            pltpu.VMEM((RING, 2 * span, rows, rows), BF16),
            pltpu.VMEM((5, rows, rows), BF16),
            pltpu.VMEM((5, rows, rows), BF16),
            pltpu.VMEM((96, rows), BF16),
            pltpu.VMEM((96, rows), BF16),
            pltpu.VMEM((2, 96, rows), F32),
            pltpu.VMEM((slots, rows), F32),
            pltpu.VMEM((8, rows), F32),
            pltpu.VMEM((8, rows), F32),
            pltpu.VMEM((6, slots, rows), F32),
            pltpu.VMEM((4, rows), F32),
        ]
        + gather_sems * 2
        + [dma((nz + nx + nc,)), dma((nz + nx + nc,)), dma((RING,)), dma((RING,))],
        compiler_params=pltpu.CompilerParams(
            collective_id=0, has_side_effects=True, vmem_limit_bytes=67043328
        ),
    )(positions, right_side, neighbours, counts[None, :])
    return out[0], out[1]


def solution(mesh):
    torus = Mesh(mesh.devices.reshape(mesh.shape["groups"], 16, 4, 2), GROUPS_BLK)
    placed = (P(None, GROUPS_BLK), P(None, GROUPS_BLK), P(None, GROUPS_BLK), P(GROUPS_BLK))
    return jax.shard_map(
        on_device,
        mesh=torus,
        in_specs=placed,
        out_specs=(P(None, GROUPS_BLK), P(None, GROUPS_BLK)),
        check_vma=False,
    )
```

```python
import functools
import math

import jax
import jax.numpy as jnp
from jax import lax
from jax.experimental import pallas as pl
from jax.experimental.pallas import tpu as pltpu
from jax.sharding import Mesh
from jax.sharding import PartitionSpec as P

REACH = 32
AXES = ("blk_0", "blk_1", "blk_2")
GROUPS_BLK = ("groups",) + AXES
MESH = pl.DeviceIdType.MESH
F32, BF16 = jnp.float32, jnp.bfloat16

SOFT = 0.0001
EPS = 1e-06
G = math.sqrt(0.75)
EDGE = 2.0 * G
FACT_A = 0.375 * G
FACT_B = 1.125 * G

RING = 4
CHUNK = 32
LOOK_Z, LOOK_X = 4, 1


def hop(k):
    return lax.div(k + 1, 2) * (2 * lax.rem(k, 2) - 1)


def total_of(x):
    return jnp.sum(jnp.sum(x, axis=1, keepdims=True), axis=0, keepdims=True)


def limbs(x, count):
    parts = []
    for k in range(count):
        part = x.astype(BF16)
        parts.append(part)
        if k < count - 1:
            x = x - part.astype(F32)
    return parts


def kernel(
    sizes, rows,
    pos_ref, rhs_ref, nbr_ref, cnt_ref,
    out_ref, a_hbm,
    blk, vec, red_c, red_x, red_z,
    keep_b, ring, stage_0, stage_1, wst_0, wst_1, acc, mult, centre, scale, lub, tot,
    spread,
    from_z1, from_x1, core_1, send_1, from_z2, from_x2, core_2, send_2, from_3, send_3,
    ring_out, ring_in,
):
    nz, nx, nc = sizes
    span = nx * nc
    tiles = nz * span
    zi, xi, ci = (lax.axis_index(a) for a in AXES)
    total = tiles * rows
    order = (zi * nx + xi) * nc + ci
    zat = lambda k: lax.rem(zi + hop(k) + nz, nz)
    xat = [lax.rem(xi + k, nx) for k in range(nx)]
    cat = [lax.rem(ci + k, nc) for k in range(nc)]
    at = lambda z, x, c: (z * nc + c) * nx + x
    me = at(zi, xi, ci)
    within = [cat[d] * nx + xat[k] for d in range(nc) for k in range(nx)]
    plus = nz // 2
    stages, wsts = (stage_0, stage_1), (wst_0, wst_1)

    barrier = pltpu.get_barrier_semaphore()
    near = []
    for step in sorted({1 % nz, nz - 1} - {0}):
        near.append({"blk_0": lax.rem(zi + step, nz)})
    near += [{"blk_1": x} for x in xat[1:]] + [{"blk_2": c} for c in cat[1:]]
    for peer in near:
        pl.semaphore_signal(barrier, inc=1, device_id=peer, device_id_type=MESH)

    ones = jnp.ones((1, rows), F32)
    blk[me] = jnp.concatenate(
        [pos_ref[...], rhs_ref[...], ones, jnp.zeros((1, rows), F32)], axis=0
    )
    middle = jnp.sum(pos_ref[...], axis=1, keepdims=True) * (1.0 / rows)
    centre[...] = jnp.concatenate(
        [jnp.broadcast_to(middle, (3, rows)), jnp.zeros((5, rows), F32)], axis=0
    )
    line = lax.broadcasted_iota(jnp.int32, (8, rows), 0)
    scale[...] = jnp.where(line < 3, G, 1.0).astype(F32)
    acc[...] = jnp.zeros(acc.shape, F32)
    pl.semaphore_wait(barrier, len(near))

    def copy(buf, s, send, recv, peer):
        return pltpu.make_async_remote_copy(
            src_ref=buf.at[s], dst_ref=buf.at[s], send_sem=send, recv_sem=recv,
            device_id=peer, device_id_type=MESH,
        )

    up = {"blk_0": lax.rem(zi + 1, nz)}
    down = {"blk_0": lax.rem(zi + nz - 1, nz)}
    beside = {"blk_2": cat[nc - 1]}

    def x_copies(buf, s, send, recv, z):
        return [copy(buf, s, send.at[1], recv.at[z], {"blk_1": x}) for x in xat[1:]]

    def c_copy(buf, send, core, z, c):
        return copy(buf, pl.ds((z * nc + c) * nx, nx), send.at[2], core.at[z], beside)

    def z_stage(buf, send, from_z, from_x, z):
        s = at(z, xi, ci)
        copy(buf, s, send.at[0], from_z.at[z], up).wait_recv()
        for c in x_copies(buf, s, send, from_x, z):
            c.start()

    def x_stage(buf, send, from_x, core, z):
        some = pl.ds((z * nc + ci) * nx, nx - 1)
        copy(buf, some, send.at[1], from_x.at[z], up).wait_recv()
        c_copy(buf, send, core, z, ci).start()

    def c_stage(buf, send, core, z):
        c_copy(buf, send, core, z, cat[nc - 1]).wait_recv()

    def relay(g, z):
        s = at(z, xi, ci)
        copy(blk, s, send_1.at[0], from_z1.at[z], up).wait_recv()
        j, odd = lax.div(g + 1, 2), lax.rem(g, 2)

        @pl.when((odd == 1) & (j < plus))
        def _():
            copy(blk, s, send_1.at[0], from_z1.at[z], down).start()

        @pl.when((odd == 0) & (j < nz - 1 - plus))
        def _():
            copy(blk, s, send_1.at[0], from_z1.at[z], up).start()

        for c in x_copies(blk, s, send_1, from_x1, z):
            c.start()

    def finish_sends(buf, send, from_z):
        for kind, count in enumerate((nz - 1, nz * (nx - 1), nz * nx)):
            copy(buf, pl.ds(0, count), send.at[kind], from_z.at[0], up).wait_send()

    own_row = (blk[me] - centre[...]) * scale[...]
    xs = [own_row[c : c + 1, :] for c in range(3)]

    def centred(s):
        return (blk[s] - centre[...]) * scale[...]

    def weights(block, vectors, out):
        along = sum(block[c : c + 1, :] * vectors[c] for c in range(3))
        columns = [
            jnp.broadcast_to(v, (8, rows)) * block for v in vectors + [along]
        ]
        for k, part in enumerate(limbs(jnp.concatenate(columns, axis=0), 3)):
            out[32 * k : 32 * (k + 1), :] = part

    def prepare(s, n):
        block = centred(s)
        raw = blk[s]
        weights(block, [raw[3 + c : 4 + c, :] for c in range(3)], wsts[n % 2])
        return block.T

    def prepare_ahead(s, n):
        turned = prepare(s, n)
        for c in range(3):
            spread[c] = jnp.broadcast_to(turned[:, c : c + 1], (rows, 128))

    def coefficients(g, slot, n, s, masked=False, ahead=False):
        stage, t = stages[n % 2], g * span + n
        turned = None if ahead else prepare(s, n)

        def put(x, k, part, keep):
            stage[k, part, :] = x.astype(BF16)
            piece = stage[k, part, :]
            keep[part, :] = piece
            return x - piece.astype(F32)

        for j in range(rows // CHUNK):
            part = slice(j * CHUNK, (j + 1) * CHUNK)
            if ahead:
                ds = [
                    jnp.concatenate([spread[c, part, :]] * (rows // 128), axis=1) - xs[c]
                    for c in range(3)
                ]
            else:
                ds = [turned[part, c : c + 1] - xs[c] for c in range(3)]
            dx, dy, dz = ds
            square = (dx * dx + dy * dy) + (dz * dz + SOFT * 0.75)
            q = lax.rsqrt(square)
            q_far = jnp.minimum(q, 1.0 / EDGE)
            q2 = q_far * q_far
            a = q_far * (q2 + 2.0) + jnp.maximum(EDGE - square * q, 0.0)
            b = (q * q2) * (2.0 / 3.0 - q2)
            if masked:
                first = lax.broadcasted_iota(jnp.int32, b.shape, 0) + j * CHUNK
                second = lax.broadcasted_iota(jnp.int32, b.shape, 1)
                b = jnp.where(first == second, 0.0, b)
            for k in range(2):
                a = put(a, k, part, ring.at[slot, 2 * n + k])
            for k in range(3):
                b = put(b, 2 + k, part, keep_b.at[t, k])

    def dot(w, m):
        return jnp.dot(w, m, preferred_element_type=F32)

    def staged(n):
        stage, w = stages[n % 2], wsts[n % 2][...]
        acc[0] += dot(w, stage[0]) + dot(w, stage[1])
        acc[1] += dot(w, stage[2]) + dot(w, stage[3]) + dot(w, stage[4])

    def ring_write(g):
        slot = lax.rem(g, RING)
        return pltpu.make_async_copy(ring.at[slot], a_hbm.at[g], ring_out.at[slot])

    def ring_read(g):
        slot = lax.rem(g, RING)
        return pltpu.make_async_copy(a_hbm.at[g], ring.at[slot], ring_in.at[slot])

    copy(blk, me, send_1.at[0], from_z1.at[zi], up).start()
    copy(blk, me, send_1.at[0], from_z1.at[zi], down).start()
    for c in x_copies(blk, me, send_1, from_x1, zi):
        c.start()
    coefficients(0, 0, 0, me, masked=True)

    own = order * rows + lax.broadcasted_iota(jnp.int32, nbr_ref.shape, 1)
    rank = lax.broadcasted_iota(jnp.int32, nbr_ref.shape, 0)
    offset = nbr_ref[...] - own + REACH
    offset = jnp.where(offset < 0, offset + total, offset)
    offset = jnp.where(offset >= total, offset - total, offset)
    offset = jnp.where(rank < cnt_ref[...], offset, -1)
    for o in range(2 * REACH + 1):
        mult[o : o + 1, :] = jnp.sum(
            jnp.where(offset == o, 1.0, 0.0), axis=0, keepdims=True
        )
    mult[2 * REACH + 1 :, :] = jnp.zeros((mult.shape[0] - 2 * REACH - 1, rows), F32)

    z_1, z_2 = (zat(jnp.int32(k)) for k in (1, 2))
    relay(jnp.int32(1), z_1)
    relay(jnp.int32(2), z_2)
    x_stage(blk, send_1, from_x1, core_1, zi)
    for n in range(1, nx):
        staged(n - 1)
        coefficients(0, 0, n, zi * span + within[n])
    c_stage(blk, send_1, core_1, zi)
    for n in range(nx, span):
        staged(n - 1)
        coefficients(0, 0, n, zi * span + within[n])
    prepare_ahead(z_1 * span + within[0], 0)
    x_stage(blk, send_1, from_x1, core_1, z_1)

    def first(g, zs):
        z_0, z_1 = zs
        z_2 = zat(g + 2)

        @pl.when(g + 2 < nz)
        def _():
            relay(g + 2, z_2)

        @pl.when(g + 1 < nz)
        def _():
            x_stage(blk, send_1, from_x1, core_1, z_1)

        c_stage(blk, send_1, core_1, z_0)

        @pl.when(g >= RING)
        def _():
            ring_write(g - RING).wait()

        slot = lax.rem(g, RING)
        for n in range(span):
            staged(n - 1)
            coefficients(g, slot, n, z_0 * span + within[n], ahead=n == 0)
            if n == 0:
                ring_write(g - 1).start()
        prepare_ahead(z_1 * span + within[0], 0)
        return z_1, z_2

    lax.fori_loop(1, nz, first, (z_1, z_2))
    staged(span - 1)

    def sums():
        out = []
        for k in range(2):
            parts = acc[k]
            out.append((parts[0:32] + parts[32:64]) + parts[64:96])
        a, b = out
        row = lambda m, r: m[r : r + 1, :]
        bv = [row(b, 8 * c + 6) for c in range(3)]
        along = sum(xs[c] * bv[c] for c in range(3)) - row(b, 30)
        far = []
        for k in range(3):
            cross = sum(xs[c] * row(b, 8 * c + k) for c in range(3))
            far.append(
                FACT_A * row(a, 8 * k + 6)
                + FACT_B * ((xs[k] * along - cross) + row(b, 24 + k))
            )
        return far

    def place(b):
        return at(lax.div(b, span), lax.rem(lax.div(b, nc), nx), lax.rem(b, nc))

    before = place(lax.rem(order + tiles - 1, tiles))
    after = place(lax.rem(order + 1, tiles))

    def lubricated(rows_of):
        def six(s):
            return jnp.concatenate([blk[s][0:3, :], rows_of(s)], axis=0)

        wide = jnp.concatenate([six(before), six(me), six(after)], axis=1)
        mine = six(me)
        for o in range(2 * REACH + 1):
            begin = rows + o - REACH
            delta = mine - wide[:, begin : begin + rows]
            for k in range(6):
                lub[k, o : o + 1, :] = delta[k : k + 1, :]
        for k in range(6):
            lub[k, 2 * REACH + 1 :, :] = jnp.zeros((lub.shape[1] - 2 * REACH - 1, rows), F32)
        d = [lub[k] for k in range(3)]
        e = [lub[3 + k] for k in range(3)]
        square = d[0] * d[0] + d[1] * d[1] + d[2] * d[2] + SOFT
        dist = jnp.sqrt(square)
        strength = mult[...] / ((0.5 + jnp.abs(dist - 2.0)) * square)
        force = strength * (d[0] * e[0] + d[1] * e[1] + d[2] * e[2])
        return [jnp.sum(force * d[k], axis=0, keepdims=True) for k in range(3)]

    rhs = [rhs_ref[k : k + 1, :] for k in range(3)]
    far = sums()
    near_part = lubricated(lambda s: blk[s][3:6, :])
    work = [far[k] + near_part[k] for k in range(3)]
    inner = lambda u, v: total_of(u[0] * v[0] + u[1] * v[1] + u[2] * v[2])
    lane = lax.broadcasted_iota(jnp.int32, (1, rows), 1)

    def packed(values):
        line = jnp.zeros((1, rows), F32)
        for k, value in enumerate(values):
            line = jnp.where(lane == k, value, line)
        return line

    def unpacked(line, count):
        return [
            jnp.sum(jnp.where(lane[:, : line.shape[1]] == k, line, 0.0), axis=1, keepdims=True)
            for k in range(count)
        ]

    vec[me] = jnp.concatenate(
        work + [packed([inner(rhs, rhs), inner(work, rhs), inner(work, work)])], axis=0
    )

    def z_copy(k):
        return copy(vec, me, send_2.at[0], from_z2.at[zi], {"blk_0": zat(k)})

    def z_start(k, _):
        z_copy(k).start()
        return 0

    for c in x_copies(vec, me, send_2, from_x2, zi):
        c.start()
    lax.fori_loop(1, nz, z_start, 0)

    def last_writes(g, _):
        ring_write(g).wait()
        return 0

    ring_write(jnp.int32(nz - 1)).start()
    acc[...] = jnp.zeros(acc.shape, F32)
    tot[...] = jnp.zeros(tot.shape, F32)

    def z_second(g):
        z_stage(vec, send_2, from_z2, from_x2, zat(g))

    def x_second(g):
        x_stage(vec, send_2, from_x2, core_2, zat(g))

    def second(g, _):
        @pl.when(g + LOOK_Z < nz)
        def _():
            z_second(g + LOOK_Z)

        @pl.when(g + LOOK_X < nz)
        def _():
            x_second(g + LOOK_X)

        z_0 = zat(g)
        c_stage(vec, send_2, core_2, z_0)
        ring_read(g).wait()
        slot = lax.rem(g, RING)
        sum_a = sum_b = None
        sum_v = tot[...]
        for n in range(span):
            s = z_0 * span + within[n]
            v = vec[s]
            sum_v = sum_v + v
            weights(centred(s), [v[c : c + 1, :] for c in range(3)], wsts[n % 2])
            w = wsts[n % 2][...]
            for k in range(2):
                part = dot(w, ring[slot, 2 * n + k])
                sum_a = part if sum_a is None else sum_a + part
            for k in range(3):
                part = dot(w, keep_b[g * span + n, k])
                sum_b = part if sum_b is None else sum_b + part
        tot[...] = sum_v
        acc[0] += sum_a
        acc[1] += sum_b

        @pl.when(g + RING < nz)
        def _():
            ring_read(g + RING).start()

        return 0

    for g in range(1, min(3, LOOK_Z, nz)):
        z_second(jnp.int32(g))
    lax.fori_loop(max(nz - RING, 0), nz, last_writes, 0)
    for g in range(min(RING, nz)):
        ring_read(jnp.int32(g)).start()
    for g in range(0, min(LOOK_X, nz)):
        x_second(jnp.int32(g))
    for g in range(3, min(LOOK_Z, nz)):
        z_second(jnp.int32(g))
    lax.fori_loop(0, nz, second, 0)

    far = sums()
    near_part = lubricated(lambda s: vec[s][0:3, :])
    again = [far[k] + near_part[k] for k in range(3)]

    rr, wr, ww = unpacked(tot[3:4, :], 3)
    beta = jnp.sqrt(rr + EPS)
    image_0 = [work[k] / beta for k in range(3)]
    v_0 = [rhs[k] / beta for k in range(3)]
    h_00 = wr / (beta * beta)
    h_10 = jnp.sqrt(ww / (beta * beta) - h_00 * h_00 + EPS)
    v_1 = [(image_0[k] - h_00 * v_0[k]) / h_10 for k in range(3)]
    image_1 = [(again[k] / beta - h_00 * image_0[k]) / h_10 for k in range(3)]
    line = packed([inner(image_1, v_0), inner(image_1, v_1), inner(image_1, image_1)])[:, :128]

    for level, (buf, mine, count, name) in enumerate(
        ((red_c, ci, nc, "blk_2"), (red_x, xi, nx, "blk_1"), (red_z, zi, nz, "blk_0"))
    ):
        others = [lax.rem(mine + k, count) for k in range(1, count)]
        buf[mine] = line
        copies = [
            copy(buf, mine, send_3.at[level], from_3.at[level], {name: other}) for other in others
        ]
        for c in copies:
            c.start()
        everyone = copy(buf, pl.ds(0, count - 1), send_3.at[level], from_3.at[level], up)
        everyone.wait_recv()
        line = buf[0]
        for k in range(1, count):
            line = line + buf[k]
        everyone.wait_send()
    h_01, h_11, squares = unpacked(line, 3)
    h_21 = jnp.sqrt(squares - h_01 * h_01 - h_11 * h_11 + EPS)

    rho_0 = jnp.sqrt(h_00 * h_00 + h_10 * h_10)
    c_0, s_0 = h_00 / rho_0, h_10 / rho_0
    g_1 = -s_0 * beta
    g_0 = c_0 * beta
    r_01 = c_0 * h_01 + s_0 * h_11
    r_11 = c_0 * h_11 - s_0 * h_01
    rho_1 = jnp.sqrt(r_11 * r_11 + h_21 * h_21)
    g_1 = (r_11 / rho_1) * g_1
    y_1 = g_1 / rho_1
    y_0 = (g_0 - r_01 * y_1) / rho_0
    for k in range(3):
        out_ref[0, k : k + 1, :] = y_0 * v_0[k] + y_1 * v_1[k]
        out_ref[1, k : k + 1, :] = rhs[k] - y_0 * image_0[k] - y_1 * image_1[k]

    finish_sends(blk, send_1, from_z1)
    finish_sends(vec, send_2, from_z2)


def on_device(positions, right_side, neighbours, counts):
    rows = positions.shape[1]
    sizes = nz, nx, nc = tuple(lax.axis_size(a) for a in AXES)
    span = nx * nc
    tiles = nz * span
    slots = 8 * -(-(2 * REACH + 1) // 8)
    vmem = pl.BlockSpec(memory_space=pltpu.VMEM)
    dma = pltpu.SemaphoreType.DMA
    gather_sems = [dma((nz,)), dma((nz,)), dma((nz,)), dma((3,))]
    out, _ = pl.pallas_call(
        functools.partial(kernel, sizes, rows),
        out_shape=(
            jax.ShapeDtypeStruct((2, 3, rows), F32),
            jax.ShapeDtypeStruct((nz, 2 * span, rows, rows), BF16),
        ),
        in_specs=[vmem] * 4,
        out_specs=(vmem, pl.BlockSpec(memory_space=pltpu.HBM)),
        scratch_shapes=[
            pltpu.VMEM((tiles, 8, rows), F32),
            pltpu.VMEM((tiles, 4, rows), F32),
            pltpu.VMEM((nc, 1, 128), F32),
            pltpu.VMEM((nx, 1, 128), F32),
            pltpu.VMEM((nz, 1, 128), F32),
            pltpu.VMEM((tiles, 3, rows, rows), BF16),
            pltpu.VMEM((RING, 2 * span, rows, rows), BF16),
            pltpu.VMEM((5, rows, rows), BF16),
            pltpu.VMEM((5, rows, rows), BF16),
            pltpu.VMEM((96, rows), BF16),
            pltpu.VMEM((96, rows), BF16),
            pltpu.VMEM((2, 96, rows), F32),
            pltpu.VMEM((slots, rows), F32),
            pltpu.VMEM((8, rows), F32),
            pltpu.VMEM((8, rows), F32),
            pltpu.VMEM((6, slots, rows), F32),
            pltpu.VMEM((4, rows), F32),
            pltpu.VMEM((3, rows, 128), F32),
        ]
        + gather_sems * 2
        + [dma((3,)), dma((3,)), dma((RING,)), dma((RING,))],
        compiler_params=pltpu.CompilerParams(
            collective_id=0, has_side_effects=True, vmem_limit_bytes=67043328
        ),
    )(positions, right_side, neighbours, counts[None, :])
    return out[0], out[1]


def solution(mesh):
    torus = Mesh(mesh.devices.reshape(mesh.shape["groups"], 16, 4, 2), GROUPS_BLK)
    placed = (P(None, GROUPS_BLK), P(None, GROUPS_BLK), P(None, GROUPS_BLK), P(GROUPS_BLK))
    return jax.shard_map(
        on_device,
        mesh=torus,
        in_specs=placed,
        out_specs=(P(None, GROUPS_BLK), P(None, GROUPS_BLK)),
        check_vma=False,
    )
```

```python
import functools
import math

import jax
import jax.numpy as jnp
from jax import lax
from jax.experimental import pallas as pl
from jax.experimental.pallas import tpu as pltpu
from jax.sharding import Mesh
from jax.sharding import PartitionSpec as P

REACH = 32
AXES = ("blk_0", "blk_1", "blk_2")
GROUPS_BLK = ("groups",) + AXES
MESH = pl.DeviceIdType.MESH
F32, BF16, F8 = jnp.float32, jnp.bfloat16, jnp.float8_e4m3fn

SOFT = 0.0001
EPS = 1e-06
K = 24.0
G = math.sqrt(0.75)
SCALE = G / K
EDGE = 2.0 * SCALE
FACT_A = 0.375 * G / K**3
FACT_B = 1.125 * G / K**3

RING = 3
CHUNK = 32
LOOK_Z, LOOK_X = 7, 2


def hop(k):
    return lax.div(k + 1, 2) * (2 * lax.rem(k, 2) - 1)


def total_of(x):
    return jnp.sum(jnp.sum(x, axis=1, keepdims=True), axis=0, keepdims=True)


def limbs(x, count):
    parts = []
    for k in range(count):
        part = x.astype(BF16)
        parts.append(part)
        if k < count - 1:
            x = x - part.astype(F32)
    return parts


def kernel(
    sizes, rows,
    pos_ref, rhs_ref, nbr_ref, cnt_ref,
    out_ref, a_hbm,
    blk, vec, red_c, red_x, red_z,
    keep, keep_8, ring, stage_0, stage_1, stage_80, stage_81, wst_0, wst_1, acc, mult, centre, scale, lub, tot,
    spread,
    from_z1, from_x1, core_1, send_1, from_z2, from_x2, core_2, send_2, from_3, send_3,
    ring_out, ring_in,
):
    nz, nx, nc = sizes
    span = nx * nc
    tiles = nz * span
    zi, xi, ci = (lax.axis_index(a) for a in AXES)
    total = tiles * rows
    order = (zi * nx + xi) * nc + ci
    zat = lambda k: lax.rem(zi + hop(k) + nz, nz)
    xat = [lax.rem(xi + k, nx) for k in range(nx)]
    cat = [lax.rem(ci + k, nc) for k in range(nc)]
    at = lambda z, x, c: (z * nc + c) * nx + x
    me = at(zi, xi, ci)
    within = [cat[d] * nx + xat[k] for d in range(nc) for k in range(nx)]
    plus = nz // 2
    stages, stages_8, wsts = (stage_0, stage_1), (stage_80, stage_81), (wst_0, wst_1)

    barrier = pltpu.get_barrier_semaphore()
    near = []
    for step in sorted({1 % nz, nz - 1} - {0}):
        near.append({"blk_0": lax.rem(zi + step, nz)})
    near += [{"blk_1": x} for x in xat[1:]] + [{"blk_2": c} for c in cat[1:]]
    for peer in near:
        pl.semaphore_signal(barrier, inc=1, device_id=peer, device_id_type=MESH)

    ones = jnp.ones((1, rows), F32)
    blk[me] = jnp.concatenate(
        [pos_ref[...], rhs_ref[...], ones, jnp.zeros((1, rows), F32)], axis=0
    )
    middle = jnp.sum(pos_ref[...], axis=1, keepdims=True) * (1.0 / rows)
    centre[...] = jnp.concatenate(
        [jnp.broadcast_to(middle, (3, rows)), jnp.zeros((5, rows), F32)], axis=0
    )
    line = lax.broadcasted_iota(jnp.int32, (8, rows), 0)
    scale[...] = jnp.where(line < 3, SCALE, 1.0).astype(F32)
    acc[...] = jnp.zeros(acc.shape, F32)
    pl.semaphore_wait(barrier, len(near))

    def copy(buf, s, send, recv, peer):
        return pltpu.make_async_remote_copy(
            src_ref=buf.at[s], dst_ref=buf.at[s], send_sem=send, recv_sem=recv,
            device_id=peer, device_id_type=MESH,
        )

    up = {"blk_0": lax.rem(zi + 1, nz)}
    down = {"blk_0": lax.rem(zi + nz - 1, nz)}
    beside = {"blk_2": cat[nc - 1]}

    def x_copies(buf, s, send, recv, z):
        return [copy(buf, s, send.at[1], recv.at[z], {"blk_1": x}) for x in xat[1:]]

    def c_copy(buf, send, core, z, c):
        return copy(buf, pl.ds((z * nc + c) * nx, nx), send.at[2], core.at[z], beside)

    def z_stage(buf, send, from_z, from_x, z):
        s = at(z, xi, ci)
        copy(buf, s, send.at[0], from_z.at[z], up).wait_recv()
        for c in x_copies(buf, s, send, from_x, z):
            c.start()

    def x_stage(buf, send, from_x, core, z):
        some = pl.ds((z * nc + ci) * nx, nx - 1)
        copy(buf, some, send.at[1], from_x.at[z], up).wait_recv()
        c_copy(buf, send, core, z, ci).start()

    def c_stage(buf, send, core, z):
        c_copy(buf, send, core, z, cat[nc - 1]).wait_recv()

    def relay(g, z):
        s = at(z, xi, ci)
        copy(blk, s, send_1.at[0], from_z1.at[z], up).wait_recv()
        j, odd = lax.div(g + 1, 2), lax.rem(g, 2)

        @pl.when((odd == 1) & (j < plus))
        def _():
            copy(blk, s, send_1.at[0], from_z1.at[z], down).start()

        @pl.when((odd == 0) & (j < nz - 1 - plus))
        def _():
            copy(blk, s, send_1.at[0], from_z1.at[z], up).start()

        for c in x_copies(blk, s, send_1, from_x1, z):
            c.start()

    def finish_sends(buf, send, from_z):
        for kind, count in enumerate((nz - 1, nz * (nx - 1), nz * nx)):
            copy(buf, pl.ds(0, count), send.at[kind], from_z.at[0], up).wait_send()

    own_row = (blk[me] - centre[...]) * scale[...]
    xs = [own_row[c : c + 1, :] for c in range(3)]

    def centred(s):
        return (blk[s] - centre[...]) * scale[...]

    def weights(block, vectors, out):
        along = sum(block[c : c + 1, :] * vectors[c] for c in range(3))
        columns = [
            jnp.broadcast_to(v, (8, rows)) * block for v in vectors + [along]
        ]
        for k, part in enumerate(limbs(jnp.concatenate(columns, axis=0), 3)):
            out[32 * k : 32 * (k + 1), :] = part

    def prepare(s, n):
        block = centred(s)
        raw = blk[s]
        weights(block, [raw[3 + c : 4 + c, :] for c in range(3)], wsts[n % 2])
        return block.T

    def prepare_ahead(s, n):
        turned = prepare(s, n)
        for c in range(3):
            spread[c] = jnp.broadcast_to(turned[:, c : c + 1], (rows, 128))

    def coefficients(g, slot, n, s, masked=False, ahead=False):
        stage, stage_8, t = stages[n % 2], stages_8[n % 2], g * span + n
        turned = None if ahead else prepare(s, n)

        def put(x, k, part):
            stage[k, part, :] = x.astype(BF16)
            piece = stage[k, part, :]
            keep[t, k, part, :] = piece
            return x - piece.astype(F32)

        def put_last(x, k, part, kept):
            stage_8[k, part, :] = x.astype(F8)
            kept[part, :] = stage_8[k, part, :]

        for j in range(rows // CHUNK):
            part = slice(j * CHUNK, (j + 1) * CHUNK)
            if ahead:
                ds = [
                    jnp.concatenate([spread[c, part, :]] * (rows // 128), axis=1) - xs[c]
                    for c in range(3)
                ]
            else:
                ds = [turned[part, c : c + 1] - xs[c] for c in range(3)]
            dx, dy, dz = ds
            square = (dx * dx + dy * dy) + (dz * dz + SOFT * SCALE * SCALE)
            q = lax.rsqrt(square)
            q_far = jnp.minimum(q, 1.0 / EDGE)
            q2 = q_far * q_far
            close = jnp.maximum(EDGE * K**4 - square * (q * K**4), 0.0)
            a = q_far * (q2 + 2.0 * K * K) + close
            b = (q * q2) * (2.0 / 3.0 * K * K - q2)
            if masked:
                first = lax.broadcasted_iota(jnp.int32, b.shape, 0) + j * CHUNK
                second = lax.broadcasted_iota(jnp.int32, b.shape, 1)
                b = jnp.where(first == second, 0.0, b)
            put_last(put(a, 0, part), 0, part, ring.at[slot, n])
            put_last(put(put(b, 1, part), 2, part), 1, part, keep_8.at[t])

    def dot(w, m):
        return jnp.dot(w, m, preferred_element_type=F32)

    def staged(n):
        stage, stage_8, w = stages[n % 2], stages_8[n % 2], wsts[n % 2][...]
        acc[0] += dot(w, stage[0]) + dot(w, stage_8[0])
        acc[1] += dot(w, stage[1]) + dot(w, stage[2]) + dot(w, stage_8[1])

    def ring_write(g):
        slot = lax.rem(g, RING)
        return pltpu.make_async_copy(ring.at[slot], a_hbm.at[g], ring_out.at[slot])

    def ring_read(g):
        slot = lax.rem(g, RING)
        return pltpu.make_async_copy(a_hbm.at[g], ring.at[slot], ring_in.at[slot])

    copy(blk, me, send_1.at[0], from_z1.at[zi], up).start()
    copy(blk, me, send_1.at[0], from_z1.at[zi], down).start()
    for c in x_copies(blk, me, send_1, from_x1, zi):
        c.start()
    coefficients(0, 0, 0, me, masked=True)

    own = order * rows + lax.broadcasted_iota(jnp.int32, nbr_ref.shape, 1)
    rank = lax.broadcasted_iota(jnp.int32, nbr_ref.shape, 0)
    offset = nbr_ref[...] - own + REACH
    offset = jnp.where(offset < 0, offset + total, offset)
    offset = jnp.where(offset >= total, offset - total, offset)
    offset = jnp.where(rank < cnt_ref[...], offset, -1)
    for o in range(2 * REACH + 1):
        mult[o : o + 1, :] = jnp.sum(
            jnp.where(offset == o, 1.0, 0.0), axis=0, keepdims=True
        )
    mult[2 * REACH + 1 :, :] = jnp.zeros((mult.shape[0] - 2 * REACH - 1, rows), F32)

    z_1, z_2 = (zat(jnp.int32(k)) for k in (1, 2))
    relay(jnp.int32(1), z_1)
    relay(jnp.int32(2), z_2)
    x_stage(blk, send_1, from_x1, core_1, zi)
    for n in range(1, nx):
        staged(n - 1)
        coefficients(0, 0, n, zi * span + within[n])
    c_stage(blk, send_1, core_1, zi)
    for n in range(nx, span):
        staged(n - 1)
        coefficients(0, 0, n, zi * span + within[n])
    prepare_ahead(z_1 * span + within[0], 0)
    x_stage(blk, send_1, from_x1, core_1, z_1)
    z_3 = zat(jnp.int32(3))
    relay(jnp.int32(3), z_3)

    def first(g, zs):
        z_0, z_1, z_2 = zs
        z_3 = zat(g + 3)

        @pl.when(g + 3 < nz)
        def _():
            relay(g + 3, z_3)

        @pl.when(g + 1 < nz)
        def _():
            x_stage(blk, send_1, from_x1, core_1, z_1)

        c_stage(blk, send_1, core_1, z_0)

        @pl.when(g >= RING)
        def _():
            ring_write(g - RING).wait()

        ring_write(g - 1).start()
        slot = lax.rem(g, RING)
        for n in range(span):
            staged(n - 1)
            coefficients(g, slot, n, z_0 * span + within[n], ahead=n == 0)
        prepare_ahead(z_1 * span + within[0], 0)
        return z_1, z_2, z_3

    lax.fori_loop(1, nz, first, (z_1, z_2, z_3))
    staged(span - 1)

    def sums():
        out = []
        for k in range(2):
            parts = acc[k]
            out.append((parts[0:32] + parts[32:64]) + parts[64:96])
        a, b = out
        row = lambda m, r: m[r : r + 1, :]
        bv = [row(b, 8 * c + 6) for c in range(3)]
        along = sum(xs[c] * bv[c] for c in range(3)) - row(b, 30)
        far = []
        for k in range(3):
            cross = sum(xs[c] * row(b, 8 * c + k) for c in range(3))
            far.append(
                FACT_A * row(a, 8 * k + 6)
                + FACT_B * ((xs[k] * along - cross) + row(b, 24 + k))
            )
        return far

    def place(b):
        return at(lax.div(b, span), lax.rem(lax.div(b, nc), nx), lax.rem(b, nc))

    before = place(lax.rem(order + tiles - 1, tiles))
    after = place(lax.rem(order + 1, tiles))

    def lubricated(rows_of):
        def six(s):
            return jnp.concatenate([blk[s][0:3, :], rows_of(s)], axis=0)

        wide = jnp.concatenate([six(before), six(me), six(after)], axis=1)
        mine = six(me)
        for o in range(2 * REACH + 1):
            begin = rows + o - REACH
            delta = mine - wide[:, begin : begin + rows]
            for k in range(6):
                lub[k, o : o + 1, :] = delta[k : k + 1, :]
        for k in range(6):
            lub[k, 2 * REACH + 1 :, :] = jnp.zeros((lub.shape[1] - 2 * REACH - 1, rows), F32)
        d = [lub[k] for k in range(3)]
        e = [lub[3 + k] for k in range(3)]
        square = d[0] * d[0] + d[1] * d[1] + d[2] * d[2] + SOFT
        dist = jnp.sqrt(square)
        strength = mult[...] / ((0.5 + jnp.abs(dist - 2.0)) * square)
        force = strength * (d[0] * e[0] + d[1] * e[1] + d[2] * e[2])
        return [jnp.sum(force * d[k], axis=0, keepdims=True) for k in range(3)]

    rhs = [rhs_ref[k : k + 1, :] for k in range(3)]
    far = sums()
    near_part = lubricated(lambda s: blk[s][3:6, :])
    work = [far[k] + near_part[k] for k in range(3)]
    inner = lambda u, v: total_of(u[0] * v[0] + u[1] * v[1] + u[2] * v[2])
    lane = lax.broadcasted_iota(jnp.int32, (1, rows), 1)

    def packed(values):
        line = jnp.zeros((1, rows), F32)
        for k, value in enumerate(values):
            line = jnp.where(lane == k, value, line)
        return line

    def unpacked(line, count):
        return [
            jnp.sum(jnp.where(lane[:, : line.shape[1]] == k, line, 0.0), axis=1, keepdims=True)
            for k in range(count)
        ]

    vec[me] = jnp.concatenate(
        work + [packed([inner(rhs, rhs), inner(work, rhs), inner(work, work)])], axis=0
    )

    def z_copy(k):
        return copy(vec, me, send_2.at[0], from_z2.at[zi], {"blk_0": zat(k)})

    def z_start(k, _):
        z_copy(k).start()
        return 0

    for c in x_copies(vec, me, send_2, from_x2, zi):
        c.start()
    lax.fori_loop(1, nz, z_start, 0)

    def last_writes(g, _):
        ring_write(g).wait()
        return 0

    ring_write(jnp.int32(nz - 1)).start()
    acc[...] = jnp.zeros(acc.shape, F32)
    tot[...] = jnp.zeros(tot.shape, F32)

    def z_second(g):
        z_stage(vec, send_2, from_z2, from_x2, zat(g))

    def x_second(g):
        x_stage(vec, send_2, from_x2, core_2, zat(g))

    def second(g, _):
        @pl.when(g + LOOK_Z < nz)
        def _():
            z_second(g + LOOK_Z)

        @pl.when(g + LOOK_X < nz)
        def _():
            x_second(g + LOOK_X)

        z_0 = zat(g)
        c_stage(vec, send_2, core_2, z_0)
        ring_read(g).wait()
        slot = lax.rem(g, RING)
        sum_a = sum_b = None
        sum_v = tot[...]
        for n in range(span):
            s = z_0 * span + within[n]
            v = vec[s]
            sum_v = sum_v + v
            weights(centred(s), [v[c : c + 1, :] for c in range(3)], wsts[n % 2])
            w = wsts[n % 2][...]
            t = g * span + n
            part = dot(w, keep[t, 0]) + dot(w, ring[slot, n])
            sum_a = part if sum_a is None else sum_a + part
            part = dot(w, keep[t, 1]) + dot(w, keep[t, 2]) + dot(w, keep_8[t])
            sum_b = part if sum_b is None else sum_b + part
        tot[...] = sum_v
        acc[0] += sum_a
        acc[1] += sum_b

        @pl.when(g + RING < nz)
        def _():
            ring_read(g + RING).start()

        return 0

    for g in range(1, min(3, LOOK_Z, nz)):
        z_second(jnp.int32(g))
    lax.fori_loop(max(nz - RING, 0), nz, last_writes, 0)
    for g in range(min(RING, nz)):
        ring_read(jnp.int32(g)).start()
    x_second(jnp.int32(0))
    for g in range(3, min(LOOK_Z, nz)):
        z_second(jnp.int32(g))
    for g in range(1, min(LOOK_X, nz)):
        x_second(jnp.int32(g))
    lax.fori_loop(0, nz, second, 0)

    far = sums()
    near_part = lubricated(lambda s: vec[s][0:3, :])
    again = [far[k] + near_part[k] for k in range(3)]

    rr, wr, ww = unpacked(tot[3:4, :], 3)
    beta = jnp.sqrt(rr + EPS)
    image_0 = [work[k] / beta for k in range(3)]
    v_0 = [rhs[k] / beta for k in range(3)]
    h_00 = wr / (beta * beta)
    h_10 = jnp.sqrt(ww / (beta * beta) - h_00 * h_00 + EPS)
    v_1 = [(image_0[k] - h_00 * v_0[k]) / h_10 for k in range(3)]
    image_1 = [(again[k] / beta - h_00 * image_0[k]) / h_10 for k in range(3)]
    line = packed([inner(image_1, v_0), inner(image_1, v_1), inner(image_1, image_1)])[:, :128]

    for level, (buf, mine, count, name) in enumerate(
        ((red_c, ci, nc, "blk_2"), (red_x, xi, nx, "blk_1"), (red_z, zi, nz, "blk_0"))
    ):
        others = [lax.rem(mine + k, count) for k in range(1, count)]
        buf[mine] = line
        copies = [
            copy(buf, mine, send_3.at[level], from_3.at[level], {name: other}) for other in others
        ]
        for c in copies:
            c.start()
        everyone = copy(buf, pl.ds(0, count - 1), send_3.at[level], from_3.at[level], up)
        everyone.wait_recv()
        line = buf[0]
        for k in range(1, count):
            line = line + buf[k]
        everyone.wait_send()
    h_01, h_11, squares = unpacked(line, 3)
    h_21 = jnp.sqrt(squares - h_01 * h_01 - h_11 * h_11 + EPS)

    rho_0 = jnp.sqrt(h_00 * h_00 + h_10 * h_10)
    c_0, s_0 = h_00 / rho_0, h_10 / rho_0
    g_1 = -s_0 * beta
    g_0 = c_0 * beta
    r_01 = c_0 * h_01 + s_0 * h_11
    r_11 = c_0 * h_11 - s_0 * h_01
    rho_1 = jnp.sqrt(r_11 * r_11 + h_21 * h_21)
    g_1 = (r_11 / rho_1) * g_1
    y_1 = g_1 / rho_1
    y_0 = (g_0 - r_01 * y_1) / rho_0
    for k in range(3):
        out_ref[0, k : k + 1, :] = y_0 * v_0[k] + y_1 * v_1[k]
        out_ref[1, k : k + 1, :] = rhs[k] - y_0 * image_0[k] - y_1 * image_1[k]

    finish_sends(blk, send_1, from_z1)
    finish_sends(vec, send_2, from_z2)


def on_device(positions, right_side, neighbours, counts):
    rows = positions.shape[1]
    sizes = nz, nx, nc = tuple(lax.axis_size(a) for a in AXES)
    span = nx * nc
    tiles = nz * span
    slots = 8 * -(-(2 * REACH + 1) // 8)
    vmem = pl.BlockSpec(memory_space=pltpu.VMEM)
    dma = pltpu.SemaphoreType.DMA
    gather_sems = [dma((nz,)), dma((nz,)), dma((nz,)), dma((3,))]
    out, _ = pl.pallas_call(
        functools.partial(kernel, sizes, rows),
        out_shape=(
            jax.ShapeDtypeStruct((2, 3, rows), F32),
            jax.ShapeDtypeStruct((nz, span, rows, rows), F8),
        ),
        in_specs=[vmem] * 4,
        out_specs=(vmem, pl.BlockSpec(memory_space=pltpu.HBM)),
        scratch_shapes=[
            pltpu.VMEM((tiles, 8, rows), F32),
            pltpu.VMEM((tiles, 4, rows), F32),
            pltpu.VMEM((nc, 1, 128), F32),
            pltpu.VMEM((nx, 1, 128), F32),
            pltpu.VMEM((nz, 1, 128), F32),
            pltpu.VMEM((tiles, 3, rows, rows), BF16),
            pltpu.VMEM((tiles, rows, rows), F8),
            pltpu.VMEM((RING, span, rows, rows), F8),
            pltpu.VMEM((3, rows, rows), BF16),
            pltpu.VMEM((3, rows, rows), BF16),
            pltpu.VMEM((2, rows, rows), F8),
            pltpu.VMEM((2, rows, rows), F8),
            pltpu.VMEM((96, rows), BF16),
            pltpu.VMEM((96, rows), BF16),
            pltpu.VMEM((2, 96, rows), F32),
            pltpu.VMEM((slots, rows), F32),
            pltpu.VMEM((8, rows), F32),
            pltpu.VMEM((8, rows), F32),
            pltpu.VMEM((6, slots, rows), F32),
            pltpu.VMEM((4, rows), F32),
            pltpu.VMEM((3, rows, 128), F32),
        ]
        + gather_sems * 2
        + [dma((3,)), dma((3,)), dma((RING,)), dma((RING,))],
        compiler_params=pltpu.CompilerParams(
            collective_id=0, has_side_effects=True, vmem_limit_bytes=67043328
        ),
    )(positions, right_side, neighbours, counts[None, :])
    return out[0], out[1]


def solution(mesh):
    torus = Mesh(mesh.devices.reshape(mesh.shape["groups"], 16, 4, 2), GROUPS_BLK)
    placed = (P(None, GROUPS_BLK), P(None, GROUPS_BLK), P(None, GROUPS_BLK), P(GROUPS_BLK))
    return jax.shard_map(
        on_device,
        mesh=torus,
        in_specs=placed,
        out_specs=(P(None, GROUPS_BLK), P(None, GROUPS_BLK)),
        check_vma=False,
    )
```
